32 devices in a mesh: groups: 2 (over y), ra: 4 (over z), dec: 2 (over x), rep: 2 (over core).
Axes of the slice: x: 2, y: 2, z: 4, core: 2. Of those that a mesh axis runs over, the one named last changes fastest.
Arguments:
- tiles: bfloat16 [2048, 16384], P(('groups', 'ra', 'dec', 'rep')), parts along dimension 0, may hold values from -6 to 6
- tile_route: int32 [2048, 1], P(('groups', 'ra', 'dec', 'rep')), parts along dimension 0, may hold values from 0 to 3; in each aligned block of 64 rows (0 to 63, 64 to 127, ...) at most 32 rows name the same one
- tile_visit: int32 [2048], P(('groups', 'ra', 'dec', 'rep')), parts along dimension 0, may hold values from 0 to 7
- tile_offset: int32 [2048], P(('groups', 'ra', 'dec', 'rep')), parts along dimension 0, may hold values from 0 to 64
- tile_weight: float32 [2048], P(('groups', 'ra', 'dec', 'rep')), parts along dimension 0, may hold values from 0.1 to 10
- resampling: bfloat16 [16, 2, 128, 128], P('groups'), parts along dimension 0, may hold values from 0 to 0.17675781
- psf_taps: float32 [16, 2, 5], P('groups'), parts along dimension 0, may hold values from 0.1 to 1
Outputs:
- coadd: float32 [512, 512], P(('groups', 'dec'), 'ra'), parts along dimension 0
- weight_map: float32 [512, 512], P(('groups', 'dec'), 'ra'), parts along dimension 0
The draws below stay inside these ranges and needn't reach their ends.
There are 2 independent parts, one for each index of `groups`. The reference program is written for one: setup_inputs(seed, part) draws one part's arguments, and reference() takes and returns one part's arrays. A program takes and returns all parts, laid end to end along the dimension named above; each array names one. Nothing has to cross between parts.
Inputs may be any that keep to these rules, and one draw needn't show every extreme that they name: `tile_route`: among the tiles of one device, at most 32 name the same RA band; in every draw some RA band is named by exactly 32 tiles of some device.
All inputs are finite; a program needn't handle non-finite values.
Results may differ from the reference program's by a relative error of at most 0.0019.
Values may be sent and summed in bfloat16 or wider, within the bound.
A program may use at most 64 MiB of HBM per device.

```python
import math
import jax
import jax.numpy as jnp
import numpy as np
from jax import lax

PIX = 128
MARGIN = 32
VISITS = 8
TILES_DEV = 64
CAP = 32
TILES_ALL = 1024
N_RA = 4
N_DEC = 2
N_REP = 2


def set_ends(values, key, smallest, top_value):
    index_at = [jax.random.randint(jax.random.fold_in(key, axis), (), 0, length) for axis, length in enumerate(values.shape)]
    main_axis = values.shape.index(max(values.shape))
    beside = index_at[:main_axis] + [(index_at[main_axis] + 1) % values.shape[main_axis]] + index_at[main_axis + 1:]
    return values.at[tuple(index_at)].set(smallest).at[tuple(beside)].set(top_value)


def shard_levels(own_key, shape, pieces, smallest, top_value):
    def one(axis_at, shards_of):
        heights = jax.random.uniform(jax.random.fold_in(jax.random.fold_in(own_key, 6), axis_at), (shards_of,), jnp.float32, smallest / len(pieces), top_value / len(pieces))
        return jnp.repeat(jnp.exp(heights), shape[axis_at] // shards_of).reshape((-1,) + (1,) * (len(shape) - axis_at - 1))

    level = one(*pieces[0])
    for cut in pieces[1:]:
        level = level * one(*cut)
    return level


def assign_block(key, own, number, rows, number_of, top, reach, skew):
    ranking = jax.random.permutation(key, number_of)
    crowded, ordinary = shares(number_of, rows * top, reach, skew, True), shares(number_of, rows * top, reach, skew, False)
    places = jnp.arange(number_of)

    def named(tallies, turn):
        used = int((tallies > 0).sum())
        fixed = max(1, used // 4)
        moved = fixed + (places - fixed + turn * (used - fixed)) % max(1, number_of - fixed)
        return jnp.zeros((number_of,), jnp.int32).at[ranking[jnp.where(places < fixed, places, moved)]].set(jnp.asarray(tallies, jnp.int32))

    tallies = jnp.where(number % 4 == 0, named(crowded, number // 4), named(ordinary, number - number // 4 - 1))
    mixed = jax.random.permutation(jax.random.fold_in(own, 3), number_of)
    donor, taker = mixed[0:number_of // 2 * 2:2], mixed[1:number_of // 2 * 2:2]
    margin = jnp.minimum(tallies[donor] - 1, reach - tallies[taker]) // 2
    margin = jnp.where((donor == ranking[0]) | (taker == ranking[0]) | (tallies[taker] == 0), 0, jnp.maximum(margin, 0))
    moved = jax.random.randint(jax.random.fold_in(own, 4), (number_of // 2,), 0, 1 << 20) % (margin + 1)
    tallies = tallies.at[donor].add(-moved).at[taker].add(moved)
    members = jnp.searchsorted(jnp.cumsum(tallies), jnp.arange(rows * top), side="right").astype(jnp.int32)
    listing = members.reshape(top, rows).T
    listing = listing[jax.random.permutation(jax.random.fold_in(own, 1), rows)]
    turn = jax.random.randint(jax.random.fold_in(own, 2), (rows, 1), 0, top)
    return jnp.take_along_axis(listing, (jnp.arange(top)[None, :] + turn) % top, axis=1)


def shares(count, total, limit, slope, full):
    portions = [(1 << 20) // math.isqrt(rank ** slope) + 1 for rank in range(1, count + 1)]
    largest = limit if full else min(limit, max(-(-total // count), total * portions[0] // sum(portions)))
    least = 1 if total - largest >= count - 1 else 0
    holding, surplus = [largest] + [least] * (count - 1), total - largest - least * (count - 1)
    while surplus > 0:
        free = [i for i in range(1, count) if holding[i] < largest] or [i for i in range(1, count) if holding[i] < limit]
        whole, budget = sum([portions[i] for i in free]), surplus
        for i in free:
            extra = min(limit - holding[i], max(1, budget * portions[i] // whole), surplus)
            holding[i] = holding[i] + extra
            surplus = surplus - extra
    return np.array(holding)


def gaussian(own_key, extent, deviation, limit, pieces=(), kind=jnp.bfloat16):
    values = deviation * jax.random.normal(own_key, extent, jnp.float32)
    if pieces:
        values = values * shard_levels(own_key, extent, pieces, -0.22, 0.18)
    return jnp.clip(values, -limit, limit).astype(kind)


def setup_inputs(seed: int = 0, part: int = 0) -> dict:
    seeds = jax.random.split(jax.random.key(seed), 8)
    part_splits = jax.random.split(jax.random.fold_in(seeds[7], part), 8)
    tiles = gaussian(part_splits[0], (TILES_ALL, PIX * PIX), 1.0, 6.0, ((0, 16),))
    tile_route_keys = jax.random.split(jax.random.fold_in(part_splits[1], 1), TILES_ALL // TILES_DEV)
    tile_route_turns = jax.random.permutation(jax.random.fold_in(part_splits[1], 3), TILES_ALL // TILES_DEV)
    tile_route = jax.vmap(lambda own, number: assign_block(jax.random.fold_in(part_splits[1], 2), own, number, TILES_DEV, N_RA, 1, CAP, 2))(tile_route_keys, tile_route_turns).reshape((TILES_ALL, 1))
    tile_visit = set_ends(jax.random.randint(part_splits[2], (TILES_ALL,), 0, VISITS), jax.random.fold_in(part_splits[2], 1), 0, VISITS - 1).astype(jnp.int32)
    tile_offset = set_ends(jax.random.randint(part_splits[3], (TILES_ALL,), 0, 2 * MARGIN + 1), jax.random.fold_in(part_splits[3], 1), 0, 2 * MARGIN).astype(jnp.int32)
    tile_weight = jnp.clip(jnp.exp(math.log(10.0) - 4.6051702 * jax.random.uniform(part_splits[4], (TILES_ALL,), jnp.float32) ** shard_levels(part_splits[4], (TILES_ALL,), ((0, 16),), -0.2, 0.2)), 0.1, 10.0)
    resampling = jnp.clip(jax.random.uniform(part_splits[5], (VISITS, 2, PIX, PIX), jnp.float32, 0.0, 0.17675781), 0.0, 0.17675781).astype(jnp.bfloat16)
    psf_taps = jnp.clip(jax.random.uniform(part_splits[6], (VISITS, 2, 5), jnp.float32, 0.1, 1.0), 0.1, 1.0)
    return {"tiles": tiles, "tile_route": tile_route, "tile_visit": tile_visit, "tile_offset": tile_offset, "tile_weight": tile_weight, "resampling": resampling, "psf_taps": psf_taps}


def convolve(image, row_taps, col_taps):
    height = image.shape[1]
    width = image.shape[2]
    padded = jnp.pad(image, ((0, 0), (2, 2), (0, 0)))
    along = jnp.zeros_like(image)
    for k in range(5):
        along = along + row_taps[:, k][:, None, None] * padded[:, k:k + height, :]
    padded = jnp.pad(along, ((0, 0), (0, 0), (2, 2)))
    result = jnp.zeros_like(image)
    for k in range(5):
        result = result + col_taps[:, k][:, None, None] * padded[:, :, k:k + width]
    return result


def render(tiles, visit, offset, resampling, psf_taps):
    count = tiles.shape[0]
    canvas_rows = PIX + 2 * MARGIN
    grid = tiles.reshape(count, PIX, PIX)
    col_maps = resampling[visit, 1]
    mid = jnp.einsum("nab,nkb->nak", grid.astype(jnp.float32), col_maps.astype(jnp.float32)).astype(jnp.bfloat16)
    row_pad = jnp.pad(resampling[:, 0], ((0, 0), (2 * MARGIN, 2 * MARGIN), (0, 0)))

    def place(v, o):
        start = (2 * MARGIN - o).astype(jnp.int32)
        return lax.dynamic_slice(row_pad, (v.astype(jnp.int32), start, jnp.int32(0)), (1, canvas_rows, PIX))[0]

    rows = jax.vmap(place)(visit, offset)
    image = jnp.einsum("nia,nak->nik", rows.astype(jnp.float32), mid.astype(jnp.float32))
    matched = convolve(image, psf_taps[visit, 0], psf_taps[visit, 1])
    row_sums = jnp.sum(rows.astype(jnp.float32), axis=2)
    col_sums = jnp.sum(col_maps.astype(jnp.float32), axis=2)
    return matched, row_sums, col_sums


def reference(tiles, tile_route, tile_visit, tile_offset, tile_weight, resampling, psf_taps):
    total = tiles.shape[0]
    per_device = total // (N_RA * N_DEC * N_REP)
    canvas_rows = PIX + 2 * MARGIN
    patches = N_RA * N_DEC
    source = jnp.arange(total, dtype=jnp.int32) // per_device
    dec_band = (source // N_REP) % N_DEC
    patch = (dec_band * N_RA + tile_route[:, 0]).astype(jnp.int32)
    block = math.gcd(total, 512)

    def step(carry, index):
        num_sum, den_sum = carry
        start = (index * block).astype(jnp.int32)

        def cut(a):
            return lax.dynamic_slice_in_dim(a, start, block, 0)

        matched, row_sums, col_sums = render(cut(tiles), cut(tile_visit), cut(tile_offset), resampling, psf_taps)
        weight = cut(tile_weight)
        which = cut(patch)
        num_sum = num_sum + jax.ops.segment_sum(weight[:, None, None] * matched, which, patches)
        foot = weight[:, None, None] * row_sums[:, :, None] * col_sums[:, None, :]
        den_sum = den_sum + jax.ops.segment_sum(foot, which, patches)
        return (num_sum, den_sum), None

    zeros = jnp.zeros((patches, canvas_rows, PIX), jnp.float32)
    (num_sum, den_sum), _ = lax.scan(step, (zeros, zeros), jnp.arange(total // block, dtype=jnp.int32))

    def fold(canvas):
        canvas = canvas.reshape(N_DEC, N_RA, canvas_rows, PIX)
        core = canvas[:, :, MARGIN:MARGIN + PIX]
        upper = canvas[:, :, MARGIN + PIX:]
        lower = canvas[:, :, :MARGIN]
        from_below = jnp.pad(upper[:-1], ((1, 0), (0, 0), (0, 0), (0, 0)))
        from_above = jnp.pad(lower[1:], ((0, 1), (0, 0), (0, 0), (0, 0)))
        core = core.at[:, :, :MARGIN].add(from_below)
        core = core.at[:, :, PIX - MARGIN:].add(from_above)
        return core

    folded_num = fold(num_sum)
    folded_den = fold(den_sum)
    coadd = folded_num / (folded_den + 1.0)

    def arrange(a):
        return a.transpose(0, 2, 1, 3).reshape(N_DEC * PIX, N_RA * PIX)

    return arrange(coadd), arrange(folded_den)
```

```python
import functools

import jax
import jax.numpy as jnp
from jax import lax
from jax.experimental import pallas as pl
from jax.experimental.pallas import tpu as pltpu
from jax.sharding import PartitionSpec as P

PIX = 128
MARGIN = 32
ROWS = PIX + 2 * MARGIN
TAPS = 5
EDGE = TAPS // 2
CHUNK = 16
SPAN = PIX + 8
WIDE = 2 * PIX
LINK = jnp.float32
MESH = pl.DeviceIdType.MESH
VMEM = pl.BlockSpec(memory_space=pltpu.VMEM)
SMEM = pl.BlockSpec(memory_space=pltpu.SMEM)
ANY = pl.BlockSpec(memory_space=pl.ANY)


def in_two(value):
    high = value.astype(jnp.bfloat16)
    return high, (value - high.astype(jnp.float32)).astype(jnp.bfloat16)


def local_kernel(
    bands, visits, tiles_hbm, route, visit, offset, weight, taps, maps,
    num_out, den_out, cols_out,
    raw, spread, mid, row_maps, col_maps, pad, row_sums, canvas, den, sems,
):
    count = tiles_hbm.shape[0]
    chunks = count // CHUNK

    def fetch(c):
        return pltpu.make_async_copy(
            tiles_hbm.at[pl.ds(c * CHUNK, CHUNK)], raw.at[c], sems.at[c]
        )

    for c in range(chunks):
        fetch(c).start()

    pad[...] = jnp.zeros_like(pad)
    canvas[...] = jnp.zeros_like(canvas)
    den[...] = jnp.zeros_like(den)
    ones = jnp.ones((8, PIX), jnp.bfloat16)
    over = (((1,), (1,)), ((), ()))

    def prepare(v, _):
        pad[0, 8 : 8 + PIX, :] = maps[v, 0].astype(jnp.float32)
        pad[1, 8 : 8 + PIX, :] = maps[v, 1].astype(jnp.float32)
        rows = jnp.zeros((SPAN, PIX), jnp.float32)
        cols = jnp.zeros((PIX, PIX), jnp.float32)
        for k in range(TAPS):
            rows += taps[k, 0, v] * pad[0, 8 + k - 2 * EDGE : 8 + k - 2 * EDGE + SPAN, :]
            cols += taps[k, 1, v] * pad[1, 8 + k - EDGE : 8 + k - EDGE + PIX, :]
        high, low = in_two(rows)
        row_maps[v, :SPAN, :PIX] = high
        row_maps[v, :SPAN, PIX : 2 * PIX] = low
        row_maps[v, :SPAN, 2 * PIX :] = high
        col_maps[v, :, :PIX], col_maps[v, :, PIX:] = in_two(cols.T)
        sums = lax.dot_general(ones, maps[v, 0], over, preferred_element_type=jnp.float32)
        row_sums[pl.ds(v, 1), :] = sums[:1]
        sums = lax.dot_general(ones, maps[v, 1], over, preferred_element_type=jnp.float32)
        cols_out[pl.ds(v, 1), :] = sums[:1]
        return 0

    lax.fori_loop(0, visits, prepare, 0)

    def work(c, _):
        fetch(c).wait()
        for a in range(PIX):
            spread[a * CHUNK : (a + 1) * CHUNK, :] = raw[c, :, a * PIX : (a + 1) * PIX].astype(
                jnp.float32
            )
        for j in range(CHUNK):
            t = c * CHUNK + j
            grid = spread[pl.ds(j, PIX, stride=CHUNK), :].astype(jnp.bfloat16)
            part = jnp.dot(grid, col_maps[visit[t]], preferred_element_type=jnp.float32)
            high, low = in_two(weight[t] * (part[:, :PIX] + part[:, PIX:]))
            mid[j, :PIX, :] = high
            mid[j, PIX : 2 * PIX, :] = high
            mid[j, 2 * PIX :, :] = low
        for j in range(CHUNK):
            t = c * CHUNK + j
            image = jnp.dot(row_maps[visit[t]], mid[j], preferred_element_type=jnp.float32)
            canvas[route[t], pl.ds(offset[t], SPAN), :] += image[:SPAN]
            line = weight[t] * row_sums[pl.ds(visit[t], 1), :]
            line = pltpu.roll(jnp.concatenate([line, jnp.zeros_like(line)], axis=1), offset[t], 1)
            at = pl.ds(route[t] * visits + visit[t], 1)
            den[0, at, :] += line[:, :PIX]
            den[1, at, :] += line[:, PIX:]
        return 0

    lax.fori_loop(0, chunks, work, 0)
    for g in range(bands):
        num_out[g] = canvas[g, EDGE : EDGE + ROWS, :].astype(num_out.dtype)
    for side in range(2):
        den_out[:, side * PIX : (side + 1) * PIX] = den[side]


def reduce_kernel(
    bands, decs, visits, num_in, den_in, cols, folded, weight_map,
    part, den_part, total, den_total, main, strip, den_strip,
    send, recv, send_den, recv_den, own, send_two, recv_two,
):
    z, x, h = lax.axis_index("ra"), lax.axis_index("dec"), lax.axis_index("rep")
    half = ROWS // 2
    barrier = pltpu.get_barrier_semaphore()
    others = [(j, k) for j in range(bands - 1, -1, -1) for k in range(2) if (j, k) != (0, 0)]

    def peer(j, k):
        return lax.rem(z + j, bands), lax.rem(h + k, 2)

    for j, k in others:
        to, core = peer(j, k)
        pl.semaphore_signal(
            barrier, inc=1, device_id={"ra": to, "rep": core}, device_id_type=MESH
        )
    for cond, to in ((x > 0, x - 1), (x < decs - 1, x + 1)):
        @pl.when(cond)
        def _():
            for core in range(2):
                pl.semaphore_signal(
                    barrier, inc=1, device_id={"dec": to, "rep": core}, device_id_type=MESH
                )
    beside = jnp.where(x > 0, 2, 0) + jnp.where(x < decs - 1, 2, 0)
    pl.semaphore_wait(barrier, len(others) + beside)

    copies = {}
    for j, k in others:
        to, core = peer(j, k)
        s = j * 2 + k
        where = {"ra": to, "rep": core}
        rows = pl.ds(pl.multiple_of(core * half, half), half)
        copies[s] = (
            pltpu.make_async_remote_copy(
                num_in.at[to, rows], part.at[s], send.at[s], recv.at[s],
                device_id=where, device_id_type=MESH,
            ),
            pltpu.make_async_remote_copy(
                den_in.at[pl.ds(pl.multiple_of(to * visits, visits), visits)],
                den_part.at[s], send_den.at[s], recv_den.at[s],
                device_id=where, device_id_type=MESH,
            ),
        )
        for copy in copies[s]:
            copy.start()
    rows = pl.ds(pl.multiple_of(h * half, half), half)
    mine = (
        pltpu.make_async_copy(num_in.at[z, rows], part.at[0], own.at[0]),
        pltpu.make_async_copy(
            den_in.at[pl.ds(pl.multiple_of(z * visits, visits), visits)], den_part.at[0], own.at[1]
        ),
    )
    for copy in mine:
        copy.start()
    for slot, cond in ((0, x == decs - 1), (1, x == 0)):
        @pl.when(cond)
        def _():
            strip[slot] = jnp.zeros(strip.shape[1:], strip.dtype)
            den_strip[slot] = jnp.zeros(den_strip.shape[1:], den_strip.dtype)

    for copy in mine:
        copy.wait()
    acc = part[0].astype(jnp.float32)
    den_acc = den_part[0]
    for s in range(1, 2 * bands):
        for copy in copies[s]:
            copy.wait_recv()
        acc += part[s].astype(jnp.float32)
        den_acc += den_part[s]
    total[...] = acc
    den_total[...] = den_acc

    own_rows = pl.ds(pl.multiple_of(MARGIN * (1 - h), MARGIN), PIX // 2)
    strip_rows = pl.ds(pl.multiple_of((PIX // 2) * h, MARGIN), MARGIN)
    across = pltpu.make_async_remote_copy(
        total.at[own_rows], main, send_two.at[4], recv_two.at[4],
        device_id={"rep": 1 - h}, device_id_type=MESH,
    )

    def to_next(core, slot, target):
        where = {"dec": target, "rep": core}
        return (
            pltpu.make_async_remote_copy(
                total.at[strip_rows], strip.at[slot], send_two.at[2 * core],
                recv_two.at[2 * slot], device_id=where, device_id_type=MESH,
            ),
            pltpu.make_async_remote_copy(
                den_total, den_strip.at[slot], send_two.at[2 * core + 1],
                recv_two.at[2 * slot + 1], device_id=where, device_id_type=MESH,
            ),
        )

    sides = ((0, (h == 0) & (x > 0), x - 1), (1, (h == 1) & (x < decs - 1), x + 1))
    for slot, cond, target in sides:
        @pl.when(cond)
        def _():
            for core in range(2):
                for copy in to_next(core, slot, target):
                    copy.start()
    across.start()

    def spread_out(lines):
        return lax.dot_general(
            lines, cols[...], (((0,), (0,)), ((), ())),
            precision=lax.Precision.HIGHEST, preferred_element_type=jnp.float32,
        )

    whole = spread_out(den_total[...])[MARGIN : MARGIN + PIX]
    folded[pl.ds(pl.multiple_of((PIX // 2) * h, MARGIN), PIX // 2), :] = total[own_rows, :]
    for slot, cond in ((0, x < decs - 1), (1, x > 0)):
        @pl.when(cond)
        def _():
            for copy in to_next(0, slot, x):
                copy.wait_recv()
    after = spread_out(den_strip[0, :, :PIX])[:MARGIN]
    before = spread_out(den_strip[1, :, PIX:])[ROWS - MARGIN - PIX : ROWS - PIX]
    across.wait_recv()
    folded[pl.ds(pl.multiple_of((PIX // 2) * (1 - h), MARGIN), PIX // 2), :] = main[...]
    low, high = PIX - MARGIN, MARGIN
    top = whole[:high] + before
    bottom = whole[low:] + after
    weight_map[:high, :] = top
    weight_map[high:low, :] = whole[high:low]
    weight_map[low:, :] = bottom
    folded[:high, :] += strip[1]
    folded[low:, :] += strip[0]

    for s in range(1, 2 * bands):
        for copy in copies[s]:
            copy.wait_send()
    across.wait_send()
    for slot, cond, target in sides:
        @pl.when(cond)
        def _():
            for core in range(2):
                for copy in to_next(core, slot, target):
                    copy.wait_send()


def divide_kernel(num, den, coadd, weight_map):
    coadd[...] = num[...] / (den[...] + 1.0)
    weight_map[...] = den[...]


def on_device(bands, decs, tiles, route, visit, offset, weight, maps, taps):
    count = tiles.shape[0]
    visits = maps.shape[0]
    half = ROWS // 2
    f32, bf16 = jnp.float32, jnp.bfloat16
    num, den, cols = pl.pallas_call(
        functools.partial(local_kernel, bands, visits),
        out_shape=(
            jax.ShapeDtypeStruct((bands, ROWS, PIX), LINK),
            jax.ShapeDtypeStruct((bands * visits, WIDE), f32),
            jax.ShapeDtypeStruct((visits, PIX), f32),
        ),
        in_specs=[ANY, SMEM, SMEM, SMEM, SMEM, SMEM, VMEM],
        out_specs=(VMEM, VMEM, VMEM),
        scratch_shapes=[
            pltpu.VMEM((count // CHUNK, CHUNK, PIX * PIX), bf16),
            pltpu.VMEM((PIX * CHUNK, PIX), f32),
            pltpu.VMEM((CHUNK, 3 * PIX, PIX), bf16),
            pltpu.VMEM((visits, SPAN + 8, 3 * PIX), bf16),
            pltpu.VMEM((visits, PIX, 2 * PIX), bf16),
            pltpu.VMEM((2, PIX + 24, PIX), f32),
            pltpu.VMEM((visits, PIX), f32),
            pltpu.VMEM((bands, 2 * MARGIN + SPAN, PIX), f32),
            pltpu.VMEM((2, bands * visits, PIX), f32),
            pltpu.SemaphoreType.DMA((count // CHUNK,)),
        ],
        name="local_sums",
    )(
        tiles, route.reshape(count), visit, offset, weight,
        taps.transpose(2, 1, 0), maps,
    )
    dma = pltpu.SemaphoreType.DMA
    cell = jax.ShapeDtypeStruct((PIX, PIX), f32)
    folded = pl.pallas_call(
        functools.partial(reduce_kernel, bands, decs, visits),
        out_shape=(cell, cell),
        in_specs=[ANY, ANY, VMEM],
        out_specs=(VMEM, VMEM),
        scratch_shapes=[
            pltpu.VMEM((2 * bands, half, PIX), LINK),
            pltpu.VMEM((2 * bands, visits, WIDE), f32),
            pltpu.VMEM((half, PIX), f32),
            pltpu.VMEM((visits, WIDE), f32),
            pltpu.VMEM((PIX // 2, PIX), f32),
            pltpu.VMEM((2, MARGIN, PIX), f32),
            pltpu.VMEM((2, visits, WIDE), f32),
            dma((2 * bands,)),
            dma((2 * bands,)),
            dma((2 * bands,)),
            dma((2 * bands,)),
            dma((2,)),
            dma((5,)),
            dma((5,)),
        ],
        compiler_params=pltpu.CompilerParams(collective_id=0, has_side_effects=True),
        name="reduce_cells",
    )(num, den, cols)
    return pl.pallas_call(
        divide_kernel,
        out_shape=(cell, cell),
        in_specs=[VMEM, VMEM],
        out_specs=(VMEM, VMEM),
        name="divide_cells",
    )(*folded)


def solution(mesh):
    spread = ("groups", "ra", "dec", "rep")
    in_specs = (
        P(spread, None),
        P(spread, None),
        P(spread),
        P(spread),
        P(spread),
        P("groups", None, None, None),
        P("groups", None, None),
    )
    out_specs = (P(("groups", "dec"), "ra"), P(("groups", "dec"), "ra"))
    return jax.shard_map(
        functools.partial(on_device, mesh.shape["ra"], mesh.shape["dec"]),
        mesh=mesh, in_specs=in_specs, out_specs=out_specs, check_vma=False,
    )
```

```python
import functools

import jax
import jax.numpy as jnp
from jax import lax
from jax.experimental import pallas as pl
from jax.experimental.pallas import tpu as pltpu
from jax.sharding import PartitionSpec as P

PIX = 128
MARGIN = 32
ROWS = PIX + 2 * MARGIN
TAPS = 5
EDGE = TAPS // 2
CHUNK = 16
SPAN = PIX + 8
WIDE = 2 * PIX
MESH = pl.DeviceIdType.MESH
VMEM = pl.BlockSpec(memory_space=pltpu.VMEM)
SMEM = pl.BlockSpec(memory_space=pltpu.SMEM)
ANY = pl.BlockSpec(memory_space=pl.ANY)


def in_two(value):
    high = value.astype(jnp.bfloat16)
    return high, (value - high.astype(jnp.float32)).astype(jnp.bfloat16)


def local_kernel(
    bands, visits, tiles_hbm, route, visit, offset, weight, taps, maps,
    num_out, den_out, cols_out,
    raw, spread, mid, row_maps, col_maps, pad, row_sums, canvas, den, sems,
):
    count = tiles_hbm.shape[0]
    chunks = count // CHUNK

    def fetch(c):
        return pltpu.make_async_copy(
            tiles_hbm.at[pl.ds(c * CHUNK, CHUNK)], raw.at[c], sems.at[c]
        )

    for c in range(chunks):
        fetch(c).start()

    pad[...] = jnp.zeros_like(pad)
    canvas[...] = jnp.zeros_like(canvas)
    den[...] = jnp.zeros_like(den)
    ones = jnp.ones((8, PIX), jnp.bfloat16)
    over = (((1,), (1,)), ((), ()))

    def prepare(v, _):
        pad[0, 8 : 8 + PIX, :] = maps[v, 0].astype(jnp.float32)
        pad[1, 8 : 8 + PIX, :] = maps[v, 1].astype(jnp.float32)
        rows = jnp.zeros((SPAN, PIX), jnp.float32)
        cols = jnp.zeros((PIX, PIX), jnp.float32)
        for k in range(TAPS):
            rows += taps[k, 0, v] * pad[0, 8 + k - 2 * EDGE : 8 + k - 2 * EDGE + SPAN, :]
            cols += taps[k, 1, v] * pad[1, 8 + k - EDGE : 8 + k - EDGE + PIX, :]
        high, low = in_two(rows)
        row_maps[v, :SPAN, :PIX] = high
        row_maps[v, :SPAN, PIX : 2 * PIX] = low
        row_maps[v, :SPAN, 2 * PIX :] = high
        col_maps[v, :, :PIX], col_maps[v, :, PIX:] = in_two(cols.T)
        sums = lax.dot_general(ones, maps[v, 0], over, preferred_element_type=jnp.float32)
        row_sums[pl.ds(v, 1), :] = sums[:1]
        sums = lax.dot_general(ones, maps[v, 1], over, preferred_element_type=jnp.float32)
        cols_out[pl.ds(v, 1), :] = sums[:1]
        return 0

    lax.fori_loop(0, visits, prepare, 0)

    def work(c, _):
        fetch(c).wait()
        for a in range(PIX):
            spread[a * CHUNK : (a + 1) * CHUNK, :] = raw[c, :, a * PIX : (a + 1) * PIX].astype(
                jnp.float32
            )
        for j in range(CHUNK):
            t = c * CHUNK + j
            grid = spread[pl.ds(j, PIX, stride=CHUNK), :].astype(jnp.bfloat16)
            part = jnp.dot(grid, col_maps[visit[t]], preferred_element_type=jnp.float32)
            high, low = in_two(weight[t] * (part[:, :PIX] + part[:, PIX:]))
            mid[j, :PIX, :] = high
            mid[j, PIX : 2 * PIX, :] = high
            mid[j, 2 * PIX :, :] = low
        for j in range(CHUNK):
            t = c * CHUNK + j
            image = jnp.dot(row_maps[visit[t]], mid[j], preferred_element_type=jnp.float32)
            canvas[route[t], pl.ds(offset[t], SPAN), :] += image[:SPAN]
            line = weight[t] * row_sums[pl.ds(visit[t], 1), :]
            line = pltpu.roll(jnp.concatenate([line, jnp.zeros_like(line)], axis=1), offset[t], 1)
            at = pl.ds(route[t] * visits + visit[t], 1)
            den[0, at, :] += line[:, :PIX]
            den[1, at, :] += line[:, PIX:]
        return 0

    lax.fori_loop(0, chunks, work, 0)
    for g in range(bands):
        num_out[g] = canvas[g, EDGE : EDGE + ROWS, :].astype(num_out.dtype)
    for side in range(2):
        den_out[:, side * PIX : (side + 1) * PIX] = den[side]


def reduce_kernel(
    bands, decs, visits, num_in, den_in, cols, folded, weight_map,
    kept, pair, sums, part, den_kept, den_pair, den_sums, den_part, total, den_total,
    main, strip, den_strip,
    own, send_pair, recv_pair, send, recv, send_den, recv_den, send_two, recv_two,
):
    z, x, h = lax.axis_index("ra"), lax.axis_index("dec"), lax.axis_index("rep")
    half = ROWS // 2
    order = sorted(range(1, bands), key=lambda j: -min(j, bands - j)) + [0]

    def band(j):
        return lax.rem(z + j, bands)

    def half_of(j, core):
        return num_in.at[band(j), pl.ds(pl.multiple_of(core * half, half), half)]

    mine = [pltpu.make_async_copy(half_of(j, h), kept.at[j], own.at[j]) for j in range(bands)]
    mine.append(pltpu.make_async_copy(den_in, den_kept, own.at[bands]))
    for copy in mine:
        copy.start()

    barrier = pltpu.get_barrier_semaphore()
    peers = [{"rep": 1 - h}] + [{"ra": band(j)} for j in range(1, bands)]
    for peer in peers:
        pl.semaphore_signal(barrier, inc=1, device_id=peer, device_id_type=MESH)
    for cond, to in ((x > 0, x - 1), (x < decs - 1, x + 1)):
        @pl.when(cond)
        def _():
            for core in range(2):
                pl.semaphore_signal(
                    barrier, inc=1, device_id={"dec": to, "rep": core}, device_id_type=MESH
                )
    beside = jnp.where(x > 0, 2, 0) + jnp.where(x < decs - 1, 2, 0)
    pl.semaphore_wait(barrier, len(peers) + beside)

    pairs = {
        j: pltpu.make_async_remote_copy(
            half_of(j, 1 - h), pair.at[j], send_pair.at[j], recv_pair.at[j],
            device_id={"rep": 1 - h}, device_id_type=MESH,
        )
        for j in order
    }
    den_copy = pltpu.make_async_remote_copy(
        den_in, den_pair, send_pair.at[bands], recv_pair.at[bands],
        device_id={"rep": 1 - h}, device_id_type=MESH,
    )
    for n, j in enumerate(order):
        pairs[j].start()
        if n == 0:
            den_copy.start()
    for slot, cond in ((0, x == decs - 1), (1, x == 0)):
        @pl.when(cond)
        def _():
            strip[slot] = jnp.zeros(strip.shape[1:], strip.dtype)
            den_strip[slot] = jnp.zeros(den_strip.shape[1:], den_strip.dtype)

    copies = {}
    for n, j in enumerate(order):
        mine[j].wait()
        pairs[j].wait_recv()
        sums[j] = kept[j] + pair[j]
        if n == 0:
            mine[bands].wait()
            den_copy.wait_recv()
            den_sums[...] = den_kept[...] + den_pair[...]
        if j == 0:
            continue
        lines = pl.ds(pl.multiple_of(band(j) * visits, visits), visits)
        where = {"ra": band(j)}
        copies[j] = (
            pltpu.make_async_remote_copy(
                sums.at[j], part.at[j], send.at[j], recv.at[j],
                device_id=where, device_id_type=MESH,
            ),
            pltpu.make_async_remote_copy(
                den_sums.at[lines], den_part.at[j], send_den.at[j], recv_den.at[j],
                device_id=where, device_id_type=MESH,
            ),
        )
        for copy in copies[j]:
            copy.start()

    acc = sums[0]
    den_acc = den_sums[pl.ds(pl.multiple_of(z * visits, visits), visits), :]
    for j in reversed(order[:-1]):
        for copy in copies[j]:
            copy.wait_recv()
        acc += part[j]
        den_acc += den_part[j]
    total[...] = acc
    den_total[...] = den_acc

    own_rows = pl.ds(pl.multiple_of(MARGIN * (1 - h), MARGIN), PIX // 2)
    strip_rows = pl.ds(pl.multiple_of((PIX // 2) * h, MARGIN), MARGIN)
    across = pltpu.make_async_remote_copy(
        total.at[own_rows], main, send_two.at[4], recv_two.at[4],
        device_id={"rep": 1 - h}, device_id_type=MESH,
    )

    def to_next(core, slot, target):
        where = {"dec": target, "rep": core}
        return (
            pltpu.make_async_remote_copy(
                total.at[strip_rows], strip.at[slot], send_two.at[2 * core],
                recv_two.at[2 * slot], device_id=where, device_id_type=MESH,
            ),
            pltpu.make_async_remote_copy(
                den_total, den_strip.at[slot], send_two.at[2 * core + 1],
                recv_two.at[2 * slot + 1], device_id=where, device_id_type=MESH,
            ),
        )

    sides = ((0, (h == 0) & (x > 0), x - 1), (1, (h == 1) & (x < decs - 1), x + 1))
    for slot, cond, target in sides:
        @pl.when(cond)
        def _():
            for core in range(2):
                for copy in to_next(core, slot, target):
                    copy.start()
    across.start()

    def spread_out(lines):
        return lax.dot_general(
            lines, cols[...], (((0,), (0,)), ((), ())),
            precision=lax.Precision.HIGHEST, preferred_element_type=jnp.float32,
        )

    whole = spread_out(den_total[...])[MARGIN : MARGIN + PIX]
    folded[pl.ds(pl.multiple_of((PIX // 2) * h, MARGIN), PIX // 2), :] = total[own_rows, :]
    for slot, cond in ((0, x < decs - 1), (1, x > 0)):
        @pl.when(cond)
        def _():
            for copy in to_next(0, slot, x):
                copy.wait_recv()
    after = spread_out(den_strip[0, :, :PIX])[:MARGIN]
    before = spread_out(den_strip[1, :, PIX:])[ROWS - MARGIN - PIX : ROWS - PIX]
    across.wait_recv()
    folded[pl.ds(pl.multiple_of((PIX // 2) * (1 - h), MARGIN), PIX // 2), :] = main[...]
    low, high = PIX - MARGIN, MARGIN
    top = whole[:high] + before
    bottom = whole[low:] + after
    weight_map[:high, :] = top
    weight_map[high:low, :] = whole[high:low]
    weight_map[low:, :] = bottom
    folded[:high, :] += strip[1]
    folded[low:, :] += strip[0]

    for j in order:
        pairs[j].wait_send()
    den_copy.wait_send()
    for j in order[:-1]:
        for copy in copies[j]:
            copy.wait_send()
    across.wait_send()
    for slot, cond, target in sides:
        @pl.when(cond)
        def _():
            for core in range(2):
                for copy in to_next(core, slot, target):
                    copy.wait_send()


def divide_kernel(num, den, coadd, weight_map):
    coadd[...] = num[...] / (den[...] + 1.0)
    weight_map[...] = den[...]


def on_device(bands, decs, tiles, route, visit, offset, weight, maps, taps):
    count = tiles.shape[0]
    visits = maps.shape[0]
    half = ROWS // 2
    f32, bf16 = jnp.float32, jnp.bfloat16
    num, den, cols = pl.pallas_call(
        functools.partial(local_kernel, bands, visits),
        out_shape=(
            jax.ShapeDtypeStruct((bands, ROWS, PIX), f32),
            jax.ShapeDtypeStruct((bands * visits, WIDE), f32),
            jax.ShapeDtypeStruct((visits, PIX), f32),
        ),
        in_specs=[ANY, SMEM, SMEM, SMEM, SMEM, SMEM, VMEM],
        out_specs=(VMEM, VMEM, VMEM),
        scratch_shapes=[
            pltpu.VMEM((count // CHUNK, CHUNK, PIX * PIX), bf16),
            pltpu.VMEM((PIX * CHUNK, PIX), f32),
            pltpu.VMEM((CHUNK, 3 * PIX, PIX), bf16),
            pltpu.VMEM((visits, SPAN + 8, 3 * PIX), bf16),
            pltpu.VMEM((visits, PIX, 2 * PIX), bf16),
            pltpu.VMEM((2, PIX + 24, PIX), f32),
            pltpu.VMEM((visits, PIX), f32),
            pltpu.VMEM((bands, 2 * MARGIN + SPAN, PIX), f32),
            pltpu.VMEM((2, bands * visits, PIX), f32),
            pltpu.SemaphoreType.DMA((count // CHUNK,)),
        ],
        name="local_sums",
    )(
        tiles, route.reshape(count), visit, offset, weight,
        taps.transpose(2, 1, 0), maps,
    )
    dma = pltpu.SemaphoreType.DMA
    cell = jax.ShapeDtypeStruct((PIX, PIX), f32)
    folded = pl.pallas_call(
        functools.partial(reduce_kernel, bands, decs, visits),
        out_shape=(cell, cell),
        in_specs=[ANY, ANY, VMEM],
        out_specs=(VMEM, VMEM),
        scratch_shapes=[
            pltpu.VMEM((bands, half, PIX), f32),
            pltpu.VMEM((bands, half, PIX), f32),
            pltpu.VMEM((bands, half, PIX), f32),
            pltpu.VMEM((bands, half, PIX), f32),
            pltpu.VMEM((bands * visits, WIDE), f32),
            pltpu.VMEM((bands * visits, WIDE), f32),
            pltpu.VMEM((bands * visits, WIDE), f32),
            pltpu.VMEM((bands, visits, WIDE), f32),
            pltpu.VMEM((half, PIX), f32),
            pltpu.VMEM((visits, WIDE), f32),
            pltpu.VMEM((PIX // 2, PIX), f32),
            pltpu.VMEM((2, MARGIN, PIX), f32),
            pltpu.VMEM((2, visits, WIDE), f32),
            dma((bands + 1,)),
            dma((bands + 1,)),
            dma((bands + 1,)),
            dma((bands,)),
            dma((bands,)),
            dma((bands,)),
            dma((bands,)),
            dma((5,)),
            dma((5,)),
        ],
        compiler_params=pltpu.CompilerParams(collective_id=0, has_side_effects=True),
        name="reduce_cells",
    )(num, den, cols)
    return pl.pallas_call(
        divide_kernel,
        out_shape=(cell, cell),
        in_specs=[VMEM, VMEM],
        out_specs=(VMEM, VMEM),
        name="divide_cells",
    )(*folded)


def solution(mesh):
    spread = ("groups", "ra", "dec", "rep")
    in_specs = (
        P(spread, None),
        P(spread, None),
        P(spread),
        P(spread),
        P(spread),
        P("groups", None, None, None),
        P("groups", None, None),
    )
    out_specs = (P(("groups", "dec"), "ra"), P(("groups", "dec"), "ra"))
    return jax.shard_map(
        functools.partial(on_device, mesh.shape["ra"], mesh.shape["dec"]),
        mesh=mesh, in_specs=in_specs, out_specs=out_specs, check_vma=False,
    )
```

```python
import functools

import jax
import jax.numpy as jnp
from jax import lax
from jax.experimental import pallas as pl
from jax.experimental.pallas import tpu as pltpu
from jax.sharding import PartitionSpec as P

PIX = 128
MARGIN = 32
ROWS = PIX + 2 * MARGIN
TAPS = 5
EDGE = TAPS // 2
CHUNK = 16
PITCH = CHUNK + 1
SPAN = PIX + 8
WIDE = 2 * PIX
MESH = pl.DeviceIdType.MESH
VMEM = pl.BlockSpec(memory_space=pltpu.VMEM)
SMEM = pl.BlockSpec(memory_space=pltpu.SMEM)
ANY = pl.BlockSpec(memory_space=pl.ANY)


def in_two(value):
    high = value.astype(jnp.bfloat16)
    return high, (value - high.astype(jnp.float32)).astype(jnp.bfloat16)


def local_kernel(
    bands, visits, tiles_hbm, route, visit, offset, weight, taps, maps,
    num_out, den_out, cols_out,
    raw, spread, mid, row_maps, col_maps, pad, row_sums, canvas, den, sems,
):
    count = tiles_hbm.shape[0]
    chunks = count // CHUNK

    def fetch(c):
        return pltpu.make_async_copy(
            tiles_hbm.at[pl.ds(c * CHUNK, CHUNK)], raw.at[c], sems.at[c]
        )

    for c in range(chunks):
        fetch(c).start()

    pad[...] = jnp.zeros_like(pad)
    canvas[...] = jnp.zeros_like(canvas)
    den[...] = jnp.zeros_like(den)
    ones = jnp.ones((8, PIX), jnp.bfloat16)
    over = (((1,), (1,)), ((), ()))

    def prepare(v, _):
        pad[0, 8 : 8 + PIX, :] = maps[v, 0].astype(jnp.float32)
        pad[1, 8 : 8 + PIX, :] = maps[v, 1].astype(jnp.float32)
        rows = jnp.zeros((SPAN, PIX), jnp.float32)
        cols = jnp.zeros((PIX, PIX), jnp.float32)
        for k in range(TAPS):
            rows += taps[k, 0, v] * pad[0, 8 + k - 2 * EDGE : 8 + k - 2 * EDGE + SPAN, :]
            cols += taps[k, 1, v] * pad[1, 8 + k - EDGE : 8 + k - EDGE + PIX, :]
        high, low = in_two(rows)
        row_maps[v, :SPAN, :PIX] = high
        row_maps[v, :SPAN, PIX : 2 * PIX] = low
        row_maps[v, :SPAN, 2 * PIX :] = high
        col_maps[v, :, :PIX], col_maps[v, :, PIX:] = in_two(cols.T)
        sums = lax.dot_general(ones, maps[v, 0], over, preferred_element_type=jnp.float32)
        row_sums[pl.ds(v, 1), :] = sums[:1]
        sums = lax.dot_general(ones, maps[v, 1], over, preferred_element_type=jnp.float32)
        cols_out[pl.ds(v, 1), :] = sums[:1]
        return 0

    lax.fori_loop(0, visits, prepare, 0)

    def work(c, _):
        fetch(c).wait()
        for a in range(PIX):
            spread[a * PITCH : a * PITCH + CHUNK, :] = raw[c, :, a * PIX : (a + 1) * PIX].astype(
                jnp.float32
            )
        for j in range(CHUNK):
            t = c * CHUNK + j
            grid = spread[pl.ds(j, PIX, stride=PITCH), :].astype(jnp.bfloat16)
            part = jnp.dot(grid, col_maps[visit[t]], preferred_element_type=jnp.float32)
            high, low = in_two(weight[t] * (part[:, :PIX] + part[:, PIX:]))
            mid[j, :PIX, :] = high
            mid[j, PIX : 2 * PIX, :] = high
            mid[j, 2 * PIX :, :] = low
        for j in range(CHUNK):
            t = c * CHUNK + j
            image = jnp.dot(row_maps[visit[t]], mid[j], preferred_element_type=jnp.float32)
            canvas[route[t], pl.ds(offset[t], SPAN), :] += image[:SPAN]
            line = weight[t] * row_sums[pl.ds(visit[t], 1), :]
            line = pltpu.roll(jnp.concatenate([line, jnp.zeros_like(line)], axis=1), offset[t], 1)
            at = pl.ds(route[t] * visits + visit[t], 1)
            den[0, at, :] += line[:, :PIX]
            den[1, at, :] += line[:, PIX:]
        return 0

    lax.fori_loop(0, chunks, work, 0)
    for g in range(bands):
        num_out[g] = canvas[g, EDGE : EDGE + ROWS, :].astype(num_out.dtype)
    for side in range(2):
        den_out[:, side * PIX : (side + 1) * PIX] = den[side]


def reduce_kernel(
    bands, decs, visits, num_in, den_in, cols, folded, weight_map,
    kept, pair, sums, part, den_kept, den_pair, den_sums, den_part, total, den_total,
    main, strip, den_strip,
    own, send_pair, recv_pair, send, recv, send_den, recv_den, send_two, recv_two,
):
    z, x, h = lax.axis_index("ra"), lax.axis_index("dec"), lax.axis_index("rep")
    half = ROWS // 2
    order = sorted(range(1, bands), key=lambda j: -min(j, bands - j)) + [0]

    def band(j):
        return lax.rem(z + j, bands)

    def half_of(j, core):
        return num_in.at[band(j), pl.ds(pl.multiple_of(core * half, half), half)]

    mine = [pltpu.make_async_copy(half_of(j, h), kept.at[j], own.at[j]) for j in range(bands)]
    mine.append(pltpu.make_async_copy(den_in, den_kept, own.at[bands]))
    for copy in mine:
        copy.start()

    barrier = pltpu.get_barrier_semaphore()
    peers = [{"rep": 1 - h}] + [{"ra": band(j)} for j in range(1, bands)]
    for peer in peers:
        pl.semaphore_signal(barrier, inc=1, device_id=peer, device_id_type=MESH)
    for cond, to in ((x > 0, x - 1), (x < decs - 1, x + 1)):
        @pl.when(cond)
        def _():
            for core in range(2):
                pl.semaphore_signal(
                    barrier, inc=1, device_id={"dec": to, "rep": core}, device_id_type=MESH
                )
    beside = jnp.where(x > 0, 2, 0) + jnp.where(x < decs - 1, 2, 0)
    pl.semaphore_wait(barrier, len(peers) + beside)

    pairs = {
        j: pltpu.make_async_remote_copy(
            half_of(j, 1 - h), pair.at[j], send_pair.at[j], recv_pair.at[j],
            device_id={"rep": 1 - h}, device_id_type=MESH,
        )
        for j in order
    }
    den_copy = pltpu.make_async_remote_copy(
        den_in, den_pair, send_pair.at[bands], recv_pair.at[bands],
        device_id={"rep": 1 - h}, device_id_type=MESH,
    )
    for n, j in enumerate(order):
        pairs[j].start()
        if n == 0:
            den_copy.start()
    for slot, cond in ((0, x == decs - 1), (1, x == 0)):
        @pl.when(cond)
        def _():
            strip[slot] = jnp.zeros(strip.shape[1:], strip.dtype)
            den_strip[slot] = jnp.zeros(den_strip.shape[1:], den_strip.dtype)

    copies = {}
    for n, j in enumerate(order):
        mine[j].wait()
        pairs[j].wait_recv()
        sums[j] = kept[j] + pair[j]
        if n == 0:
            mine[bands].wait()
            den_copy.wait_recv()
            den_sums[...] = den_kept[...] + den_pair[...]
        if j == 0:
            continue
        lines = pl.ds(pl.multiple_of(band(j) * visits, visits), visits)
        where = {"ra": band(j)}
        copies[j] = (
            pltpu.make_async_remote_copy(
                sums.at[j], part.at[j], send.at[j], recv.at[j],
                device_id=where, device_id_type=MESH,
            ),
            pltpu.make_async_remote_copy(
                den_sums.at[lines], den_part.at[j], send_den.at[j], recv_den.at[j],
                device_id=where, device_id_type=MESH,
            ),
        )
        for copy in copies[j]:
            copy.start()

    acc = sums[0]
    den_acc = den_sums[pl.ds(pl.multiple_of(z * visits, visits), visits), :]
    for j in reversed(order[:-1]):
        for copy in copies[j]:
            copy.wait_recv()
        acc += part[j]
        den_acc += den_part[j]
    total[...] = acc
    den_total[...] = den_acc

    own_rows = pl.ds(pl.multiple_of(MARGIN * (1 - h), MARGIN), PIX // 2)
    strip_rows = pl.ds(pl.multiple_of((PIX // 2) * h, MARGIN), MARGIN)
    across = pltpu.make_async_remote_copy(
        total.at[own_rows], main, send_two.at[4], recv_two.at[4],
        device_id={"rep": 1 - h}, device_id_type=MESH,
    )

    def to_next(core, slot, target):
        where = {"dec": target, "rep": core}
        return (
            pltpu.make_async_remote_copy(
                total.at[strip_rows], strip.at[slot], send_two.at[2 * core],
                recv_two.at[2 * slot], device_id=where, device_id_type=MESH,
            ),
            pltpu.make_async_remote_copy(
                den_total, den_strip.at[slot], send_two.at[2 * core + 1],
                recv_two.at[2 * slot + 1], device_id=where, device_id_type=MESH,
            ),
        )

    sides = ((0, (h == 0) & (x > 0), x - 1), (1, (h == 1) & (x < decs - 1), x + 1))
    for slot, cond, target in sides:
        @pl.when(cond)
        def _():
            for core in range(2):
                for copy in to_next(core, slot, target):
                    copy.start()
    across.start()

    def spread_out(lines):
        return lax.dot_general(
            lines, cols[...], (((0,), (0,)), ((), ())),
            precision=lax.Precision.HIGHEST, preferred_element_type=jnp.float32,
        )

    whole = spread_out(den_total[...])[MARGIN : MARGIN + PIX]
    folded[pl.ds(pl.multiple_of((PIX // 2) * h, MARGIN), PIX // 2), :] = total[own_rows, :]
    for slot, cond in ((0, x < decs - 1), (1, x > 0)):
        @pl.when(cond)
        def _():
            for copy in to_next(0, slot, x):
                copy.wait_recv()
    after = spread_out(den_strip[0, :, :PIX])[:MARGIN]
    before = spread_out(den_strip[1, :, PIX:])[ROWS - MARGIN - PIX : ROWS - PIX]
    across.wait_recv()
    folded[pl.ds(pl.multiple_of((PIX // 2) * (1 - h), MARGIN), PIX // 2), :] = main[...]
    low, high = PIX - MARGIN, MARGIN
    top = whole[:high] + before
    bottom = whole[low:] + after
    weight_map[:high, :] = top
    weight_map[high:low, :] = whole[high:low]
    weight_map[low:, :] = bottom
    folded[:high, :] += strip[1]
    folded[low:, :] += strip[0]

    for j in order:
        pairs[j].wait_send()
    den_copy.wait_send()
    for j in order[:-1]:
        for copy in copies[j]:
            copy.wait_send()
    across.wait_send()
    for slot, cond, target in sides:
        @pl.when(cond)
        def _():
            for core in range(2):
                for copy in to_next(core, slot, target):
                    copy.wait_send()


def divide_kernel(num, den, coadd, weight_map):
    coadd[...] = num[...] / (den[...] + 1.0)
    weight_map[...] = den[...]


def on_device(bands, decs, tiles, route, visit, offset, weight, maps, taps):
    count = tiles.shape[0]
    visits = maps.shape[0]
    half = ROWS // 2
    f32, bf16 = jnp.float32, jnp.bfloat16
    num, den, cols = pl.pallas_call(
        functools.partial(local_kernel, bands, visits),
        out_shape=(
            jax.ShapeDtypeStruct((bands, ROWS, PIX), f32),
            jax.ShapeDtypeStruct((bands * visits, WIDE), f32),
            jax.ShapeDtypeStruct((visits, PIX), f32),
        ),
        in_specs=[ANY, SMEM, SMEM, SMEM, SMEM, SMEM, VMEM],
        out_specs=(VMEM, VMEM, VMEM),
        scratch_shapes=[
            pltpu.VMEM((count // CHUNK, CHUNK, PIX * PIX), bf16),
            pltpu.VMEM((PIX * PITCH, PIX), f32),
            pltpu.VMEM((CHUNK, 3 * PIX, PIX), bf16),
            pltpu.VMEM((visits, SPAN + 8, 3 * PIX), bf16),
            pltpu.VMEM((visits, PIX, 2 * PIX), bf16),
            pltpu.VMEM((2, PIX + 24, PIX), f32),
            pltpu.VMEM((visits, PIX), f32),
            pltpu.VMEM((bands, 2 * MARGIN + SPAN, PIX), f32),
            pltpu.VMEM((2, bands * visits, PIX), f32),
            pltpu.SemaphoreType.DMA((count // CHUNK,)),
        ],
        name="local_sums",
    )(
        tiles, route.reshape(count), visit, offset, weight,
        taps.transpose(2, 1, 0), maps,
    )
    dma = pltpu.SemaphoreType.DMA
    cell = jax.ShapeDtypeStruct((PIX, PIX), f32)
    folded = pl.pallas_call(
        functools.partial(reduce_kernel, bands, decs, visits),
        out_shape=(cell, cell),
        in_specs=[ANY, ANY, VMEM],
        out_specs=(VMEM, VMEM),
        scratch_shapes=[
            pltpu.VMEM((bands, half, PIX), f32),
            pltpu.VMEM((bands, half, PIX), f32),
            pltpu.VMEM((bands, half, PIX), f32),
            pltpu.VMEM((bands, half, PIX), f32),
            pltpu.VMEM((bands * visits, WIDE), f32),
            pltpu.VMEM((bands * visits, WIDE), f32),
            pltpu.VMEM((bands * visits, WIDE), f32),
            pltpu.VMEM((bands, visits, WIDE), f32),
            pltpu.VMEM((half, PIX), f32),
            pltpu.VMEM((visits, WIDE), f32),
            pltpu.VMEM((PIX // 2, PIX), f32),
            pltpu.VMEM((2, MARGIN, PIX), f32),
            pltpu.VMEM((2, visits, WIDE), f32),
            dma((bands + 1,)),
            dma((bands + 1,)),
            dma((bands + 1,)),
            dma((bands,)),
            dma((bands,)),
            dma((bands,)),
            dma((bands,)),
            dma((5,)),
            dma((5,)),
        ],
        compiler_params=pltpu.CompilerParams(collective_id=0, has_side_effects=True),
        name="reduce_cells",
    )(num, den, cols)
    return pl.pallas_call(
        divide_kernel,
        out_shape=(cell, cell),
        in_specs=[VMEM, VMEM],
        out_specs=(VMEM, VMEM),
        name="divide_cells",
    )(*folded)


def solution(mesh):
    spread = ("groups", "ra", "dec", "rep")
    in_specs = (
        P(spread, None),
        P(spread, None),
        P(spread),
        P(spread),
        P(spread),
        P("groups", None, None, None),
        P("groups", None, None),
    )
    out_specs = (P(("groups", "dec"), "ra"), P(("groups", "dec"), "ra"))
    return jax.shard_map(
        functools.partial(on_device, mesh.shape["ra"], mesh.shape["dec"]),
        mesh=mesh, in_specs=in_specs, out_specs=out_specs, check_vma=False,
    )
```
